32 devices in a mesh: comm: 4 (over z), arc: 8 (over y, x, core).
Axes of the slice: x: 2, y: 2, z: 4, core: 2. Of those that a mesh axis runs over, the one named last changes fastest.
Arguments:
- prev_dist: float32 [512, 2048], P('comm', 'arc'), may hold values from 0 to 4
- source_node: int32 [512], P('comm'), may hold values from 0 to 2047, as said below
- arc_tail: int32 [16, 2048], P(None, 'arc'), may hold values from 0 to 2047, as said below
- base_cost: float32 [16, 2048], P(None, 'arc'), may hold values from 0.05 to 1
- arc_price: float32 [16, 2048], P(None, 'arc'), may hold values from 0 to 1
- capacity: float32 [16, 2048], P(None, 'arc')
- path_arcs: int32 [512, 128], P(('comm', 'arc')), may hold values from 0 to 32767, as said below
- demand: float32 [512], P(('comm', 'arc')), may hold values from 0.5 to 2
Outputs:
- final_dist: float32 [512, 2048], P('comm', 'arc')
- new_price: float32 [16, 2048], P(None, 'arc')
The draws below stay inside these ranges and needn't reach their ends.
Inputs may be any that keep to these rules, and one draw needn't show every extreme that they name: `arc_tail`: the tail of arc s * 2048 + v lies in a node block (nodes 128 b to 128 b + 127) at most 2 blocks before or after v's block, counted around the cycle of blocks. Row k is a walk: the head of path_arcs[k, h + 1] (its id modulo 2048) is the tail of path_arcs[k, h]. `source_node`: the tail of path_arcs[k, 127].
All inputs are finite; a program needn't handle non-finite values.
Results may differ from the reference program's by a relative error of at most 0.00002.
Values sent between devices are 32-bit elements; how exact they have to be, the bound alone decides.
A program may use at most 64 MiB of HBM per device.

```python
import math
import jax
import jax.numpy as jnp
from jax import lax

LANES = 128
BLK_DEV = 2
IN_DEG = 16
SWEEPS = 8
HOPS = 128
NODES = 2048
K = 512


def make_tails(key):
    tail_key = jax.random.fold_in(key, 11)
    key_pair = jax.random.split(tail_key, 2)
    head_nodes = jnp.arange(NODES, dtype=jnp.int32)
    head_block = head_nodes // LANES
    blocks_all = NODES // LANES
    offset = jax.random.randint(key_pair[0], (IN_DEG, NODES), -BLK_DEV, BLK_DEV + 1)
    lane_pick = jax.random.randint(key_pair[1], (IN_DEG, NODES), 0, LANES)
    return (jnp.mod(head_block[None, :] + offset, blocks_all) * LANES + lane_pick).astype(jnp.int32)


def make_walks(key):
    tail_nodes = make_tails(key).reshape(-1)
    walk_key = jax.random.fold_in(key, 23)
    key_pair = jax.random.split(walk_key, 2)
    sink_nodes = jax.random.randint(key_pair[0], (K,), 0, NODES).astype(jnp.int32)
    slot_picks = jax.random.randint(key_pair[1], (HOPS, K), 0, IN_DEG).astype(jnp.int32)

    def advance(current, picked):
        arc_ids = picked * NODES + current
        return (tail_nodes[arc_ids], arc_ids)
    endpoint, walked = lax.scan(advance, sink_nodes, slot_picks)
    return (walked.T.astype(jnp.int32), endpoint.astype(jnp.int32))


def draw_arc_tail(key, part):
    return make_tails(key)


def draw_path_arcs(key, part):
    return make_walks(key)[0]


def draw_source_node(key, part):
    return make_walks(key)[1]


def draw_capacity(key, part):
    mean_load = K * HOPS / (IN_DEG * NODES)
    positions = jnp.arange(NODES, dtype=jnp.float32) / NODES
    rough_factor = jnp.exp(jax.random.uniform(key, (IN_DEG, NODES), jnp.float32, math.log(0.3), math.log(3.0)))
    return (mean_load * rough_factor * (0.5 + 1.5 * positions)[None, :]).astype(jnp.float32)


def block_scale(own_key, dims, pieces, least, largest):
    loudness = 1.0
    for dim, parts in pieces:
        heights = jax.random.uniform(jax.random.fold_in(jax.random.fold_in(own_key, 6), dim), (parts,), jnp.float32, least / len(pieces), largest / len(pieces))
        loudness = loudness * jnp.repeat(jnp.exp(heights), dims[dim] // parts).reshape((-1,) + (1,) * (len(dims) - 1 - dim))
    return loudness


def setup_inputs(seed: int = 0) -> dict:
    key_of = jax.random.split(jax.random.key(seed), 9)
    return {
        "prev_dist": jnp.clip(4.0 * jax.random.uniform(key_of[0], (K, NODES), jnp.float32) ** block_scale(key_of[0], (K, NODES), ((0, 4), (1, 8)), -0.2, 0.2), 0.0, 4.0),
        "source_node": draw_source_node(jax.random.fold_in(key_of[8], 71), 0),
        "arc_tail": draw_arc_tail(jax.random.fold_in(key_of[8], 71), 0),
        "base_cost": jnp.clip(jnp.exp(math.log(1.0) - 2.9957323 * jax.random.uniform(key_of[3], (IN_DEG, NODES), jnp.float32) ** block_scale(key_of[3], (IN_DEG, NODES), ((1, 8),), -0.2, 0.2)), 0.05, 1.0),
        "arc_price": jnp.clip(1.0 * jax.random.uniform(key_of[4], (IN_DEG, NODES), jnp.float32) ** block_scale(key_of[4], (IN_DEG, NODES), ((1, 8),), -0.2, 0.2), 0.0, 1.0),
        "capacity": draw_capacity(jax.random.fold_in(key_of[8], 71), 0),
        "path_arcs": draw_path_arcs(jax.random.fold_in(key_of[8], 71), 0),
        "demand": jnp.clip(jnp.exp(math.log(2.0) - 1.3862944 * jax.random.uniform(key_of[7], (K,), jnp.float32) ** block_scale(key_of[7], (K,), ((0, 32),), -0.2, 0.2)), 0.5, 2.0),
    }


step_size = 0.25
eps_value = 1e-06

def reference(prev_dist, source_node, arc_tail, base_cost, arc_price, capacity, path_arcs, demand):
    arc_weight = base_cost + arc_price
    node_ids = jnp.arange(NODES, dtype=jnp.int32)
    distance = jnp.where(node_ids[None, :] == source_node[:, None], jnp.float32(0.0), prev_dist)
    for sweep_number in range(SWEEPS):
        best_dist = distance
        for in_slot in range(IN_DEG):
            candidate = jnp.take(distance, arc_tail[in_slot], axis=1) + arc_weight[in_slot][None, :]
            best_dist = jnp.minimum(best_dist, candidate)
        distance = best_dist
    amounts = jnp.broadcast_to(demand[:, None], path_arcs.shape).reshape(-1)
    flattened = jnp.zeros((IN_DEG * NODES,), jnp.float32).at[path_arcs.reshape(-1)].add(amounts)
    arc_flow = flattened.reshape(IN_DEG, NODES)
    gradient = arc_flow - capacity
    scale_root = jnp.sqrt(jnp.sum(gradient * gradient) / (IN_DEG * NODES) + eps_value)
    new_price = jnp.maximum(arc_price + step_size * gradient / scale_root, jnp.float32(0.0))
    return (distance, new_price)
```

```python
import functools

import jax
import jax.numpy as jnp
from jax import lax
from jax.experimental import pallas as pl
from jax.experimental.pallas import tpu as pltpu
from jax.sharding import PartitionSpec as P

SWEEPS = 8
LANES = 128
REACH = 2
UNROLL = 2

step_size = 0.25
eps_value = 1e-06
MESH_ID = pl.DeviceIdType.MESH


def kernel(A, C, m,
           source_ref, demand_ref, dist_ref, tail_ref, cost_ref, price_ref, cap_ref, path_ref,
           out_ref, newp_ref,
           D, T, W, CODE, F, RF, G, Q,
           d_s, d_r, t_s, t_r, w_s, w_r, f_s, f_r, g_s, g_r, q_s, q_r, o_s, o_r):
    rows = D.shape[2]
    degree, span = tail_ref.shape
    NB = A * m
    node_count = NB * LANES
    me = lax.axis_index("arc")
    mc = lax.axis_index("comm")

    def arc_dev(i):
        return lax.rem(me + i, A)

    def comm_dev(i):
        return lax.rem(mc + i, C)

    W[me] = cost_ref[...] + price_ref[...]
    T[me] = tail_ref[...]
    D[0, me] = dist_ref[me]

    barrier = pltpu.get_barrier_semaphore()
    for i in range(1, A):
        pl.semaphore_signal(barrier, inc=1, device_id=(mc, arc_dev(i)), device_id_type=MESH_ID)
    for i in range(1, C):
        pl.semaphore_signal(barrier, inc=1, device_id=(comm_dev(i), me), device_id_type=MESH_ID)
    pl.semaphore_wait(barrier, A - 1 + C - 1)

    def send(src, dst, ss, rs, dev):
        return pltpu.make_async_remote_copy(src_ref=src, dst_ref=dst, send_sem=ss, recv_sem=rs,
                                            device_id=dev, device_id_type=MESH_ID)

    bulk = []
    for i in range(1, A):
        j = arc_dev(i)
        dev = (mc, j)
        bulk.append(send(tail_ref, T.at[me], t_s.at[i - 1], t_r.at[i - 1], dev))
        bulk.append(send(dist_ref.at[j], D.at[0, me], d_s.at[i - 1], d_r.at[i - 1], dev))
        bulk.append(send(W.at[me], W.at[me], w_s.at[i - 1], w_r.at[i - 1], dev))
    for c in bulk:
        c.start()

    total_rows = NB * degree
    shift_nodes = (node_count - 1).bit_length()
    assert 1 << shift_nodes == node_count
    path = path_ref[...]
    slot_of = path >> shift_nodes
    node_of = path & (node_count - 1)
    row_of = (node_of >> 7) * degree + slot_of
    lane_of = node_of & (LANES - 1)
    row_iota = lax.broadcasted_iota(jnp.int32, (total_rows, LANES), 0)
    lane_iota = lax.broadcasted_iota(jnp.int32, (LANES, LANES), 0)
    acc = jnp.zeros((total_rows, LANES), jnp.float32)
    for k in range(path.shape[0]):
        hi = jnp.where(row_iota == row_of[k:k + 1, :], 1.0, 0.0).astype(jnp.bfloat16)
        lo = jnp.where(lane_iota == lane_of[k:k + 1, :], 1.0, 0.0).astype(jnp.bfloat16)
        count = lax.dot_general(hi, lo, (((1,), (1,)), ((), ())), preferred_element_type=jnp.float32)
        acc = acc + count * demand_ref[k]
    F[...] = acc.reshape(F.shape)

    for c in bulk:
        c.wait_recv()

    sub_iota = lax.broadcasted_iota(jnp.int32, (rows, LANES), 0)
    lane_row = lax.broadcasted_iota(jnp.int32, (rows, LANES), 1)
    source = jnp.zeros((rows, LANES), jnp.int32)
    for r in range(rows):
        source = jnp.where(sub_iota == r, source_ref[me * rows + r], source)
    def prepare(j, _):
        for h in range(m):
            lanes = slice(h * LANES, (h + 1) * LANES)
            vb = j * m + h
            D[0, j, :, lanes] = jnp.where(lane_row + vb * LANES == source, 0.0, D[0, j, :, lanes])
            tail = T[j, :, lanes]
            rel = (tail >> 7) - vb + REACH
            rel = jnp.where(rel < 0, rel + NB, rel)
            rel = jnp.where(rel >= NB, rel - NB, rel)
            CODE[j, :, lanes] = rel
            T[j, :, lanes] = tail & (LANES - 1)
        return 0

    for c in bulk:
        c.wait_send()
    lax.fori_loop(0, A, prepare, 0)

    flows = []
    for i in range(1, A):
        j = arc_dev(i)
        flows.append(send(F.at[j], RF.at[me], f_s.at[i - 1], f_r.at[i - 1], (mc, j)))
    for c in flows:
        c.start()

    chunks = [slice(r, min(r + 8, rows)) for r in range(0, rows, 8)]

    def relax_block(read, write, j):
        for h in range(m):
            lanes = slice(h * LANES, (h + 1) * LANES)
            srcs = []
            for off in range(-REACH, REACH + 1):
                q = h + off
                jj = lax.rem(j + (q // m) % A, A)
                blk = q % m
                srcs.append([D[read, jj, ch, blk * LANES:(blk + 1) * LANES] for ch in chunks])
            best = list(srcs[REACH])
            for s in range(degree):
                for n, ch in enumerate(chunks):
                    shape = best[n].shape
                    idx = jnp.broadcast_to(T[j, s:s + 1, lanes], shape)
                    code = jnp.broadcast_to(CODE[j, s:s + 1, lanes], shape)
                    w = jnp.broadcast_to(W[j, s:s + 1, lanes], shape)
                    got = [jnp.take_along_axis(srcs[b][n], idx, axis=1, mode="promise_in_bounds")
                           for b in range(2 * REACH + 1)]
                    pick = got[2 * REACH]
                    for b in range(2 * REACH):
                        pick = jnp.where(code == b, got[b], pick)
                    best[n] = jnp.minimum(best[n], pick + w)
            for n, ch in enumerate(chunks):
                D[write, j, ch, lanes] = best[n]

    def sweeps(first, last):
        def one(t, _):
            read = lax.rem(t, 2)
            def blk(j, _):
                relax_block(read, 1 - read, j)
                return 0
            lax.fori_loop(0, A, blk, 0, unroll=UNROLL)
            return 0
        lax.fori_loop(first, last, one, 0)

    sweeps(0, 2)
    for c in flows:
        c.wait()
    total = F[me]
    for i in range(1, A):
        total = total + RF[arc_dev(i)]
    G[mc] = total
    sweeps(2, 3)
    groups = [send(G.at[mc], G.at[mc], g_s.at[i - 1], g_r.at[i - 1], (comm_dev(i), me)) for i in range(1, C)]
    for c in groups:
        c.start()
    sweeps(3, 5)
    for c in groups:
        c.wait()
    flow = G[0]
    for i in range(1, C):
        flow = flow + G[i]
    gradient = [flow[h * degree:(h + 1) * degree, :] - cap_ref[:, h * LANES:(h + 1) * LANES] for h in range(m)]
    square = sum(g * g for g in gradient)
    Q[me] = square
    sweeps(5, 6)
    norms = [send(Q.at[me], Q.at[me], q_s.at[i - 1], q_r.at[i - 1], (mc, arc_dev(i))) for i in range(1, A)]
    for c in norms:
        c.start()
    sweeps(6, SWEEPS - 1)
    for c in norms:
        c.wait()
    square = Q[0]
    for i in range(1, A):
        square = square + Q[i]
    scale_root = jnp.sqrt(jnp.sum(square) / (degree * node_count) + eps_value)
    for h in range(m):
        lanes = slice(h * LANES, (h + 1) * LANES)
        newp_ref[:, lanes] = jnp.maximum(price_ref[:, lanes] + step_size * gradient[h] / scale_root, 0.0)

    read = (SWEEPS - 1) % 2
    outs = [send(D.at[1 - read, arc_dev(i)], out_ref.at[me], o_s.at[i - 1], o_r.at[i - 1], (mc, arc_dev(i)))
            for i in range(1, A)]
    for i in range(1, A + 1):
        relax_block(read, 1 - read, arc_dev(i))
        if i >= 2:
            outs[i - 2].start()
    out_ref[me] = D[1 - read, me]
    for c in outs:
        c.wait()


def shards(A, C, prev_dist, source_node, arc_tail, base_cost, arc_price, capacity, path_arcs, demand):
    commodities, span = prev_dist.shape
    degree = arc_tail.shape[0]
    rows = commodities // A
    m = span // LANES
    f32 = jnp.float32
    vmem = pl.BlockSpec(memory_space=pltpu.VMEM)
    smem = pl.BlockSpec(memory_space=pltpu.SMEM)
    sems = pltpu.SemaphoreType.DMA
    out, new_price = pl.pallas_call(
        functools.partial(kernel, A, C, m),
        out_shape=(jax.ShapeDtypeStruct((A, rows, span), f32), jax.ShapeDtypeStruct((degree, span), f32)),
        in_specs=[smem, smem] + [vmem] * 6,
        out_specs=(vmem, vmem),
        scratch_shapes=[
            pltpu.VMEM((2, A, rows, span), f32),
            pltpu.VMEM((A, degree, span), jnp.int32),
            pltpu.VMEM((A, degree, span), f32),
            pltpu.VMEM((A, degree, span), jnp.int32),
            pltpu.VMEM((A, m * degree, LANES), f32),
            pltpu.VMEM((A, m * degree, LANES), f32),
            pltpu.VMEM((C, m * degree, LANES), f32),
            pltpu.VMEM((A, degree, LANES), f32),
        ] + [sems((A - 1,))] * 8 + [sems((C - 1,))] * 2 + [sems((A - 1,))] * 4,
        compiler_params=pltpu.CompilerParams(collective_id=0, has_side_effects=True),
    )(source_node, demand, prev_dist.reshape(A, rows, span), arc_tail, base_cost, arc_price, capacity, path_arcs)
    return (out.reshape(commodities, span), new_price)


def solution(mesh):
    in_specs = (
        P("comm", "arc"),
        P("comm"),
        P(None, "arc"),
        P(None, "arc"),
        P(None, "arc"),
        P(None, "arc"),
        P(("comm", "arc"), None),
        P(("comm", "arc")),
    )
    out_specs = (P("comm", "arc"), P(None, "arc"))
    body = functools.partial(shards, mesh.shape["arc"], mesh.shape["comm"])
    return jax.shard_map(body, mesh=mesh, in_specs=in_specs, out_specs=out_specs, check_vma=False)
```

```python
import functools

import jax
import jax.numpy as jnp
from jax import lax
from jax.experimental import pallas as pl
from jax.experimental.pallas import tpu as pltpu
from jax.sharding import PartitionSpec as P

SWEEPS = 8
LANES = 128
REACH = 2
UNROLL = 2

step_size = 0.25
eps_value = 1e-06
MESH_ID = pl.DeviceIdType.MESH


def kernel(A, C, m,
           source_ref, demand_ref, dist_ref, tail_ref, cost_ref, price_ref, cap_ref, path_ref,
           out_ref, newp_ref,
           D, T, W, CODE, F, RF, G, Q,
           d_s, d_r, t_s, t_r, w_s, w_r, f_s, f_r, g_s, g_r, q_s, q_r, o_s, o_r):
    rows = D.shape[2]
    degree, span = tail_ref.shape
    NB = A * m
    node_count = NB * LANES
    me = lax.axis_index("arc")
    mc = lax.axis_index("comm")

    def arc_dev(i):
        return lax.rem(me + i, A)

    def comm_dev(i):
        return lax.rem(mc + i, C)

    W[me] = cost_ref[...] + price_ref[...]
    T[me] = tail_ref[...]
    D[0, me] = dist_ref[me]

    barrier = pltpu.get_barrier_semaphore()
    for i in range(1, A):
        pl.semaphore_signal(barrier, inc=1, device_id=(mc, arc_dev(i)), device_id_type=MESH_ID)
    for i in range(1, C):
        pl.semaphore_signal(barrier, inc=1, device_id=(comm_dev(i), me), device_id_type=MESH_ID)
    pl.semaphore_wait(barrier, A - 1 + C - 1)

    def send(src, dst, ss, rs, dev):
        return pltpu.make_async_remote_copy(src_ref=src, dst_ref=dst, send_sem=ss, recv_sem=rs,
                                            device_id=dev, device_id_type=MESH_ID)

    bulk = []
    for i in range(1, A):
        j = arc_dev(i)
        dev = (mc, j)
        bulk.append(send(tail_ref, T.at[me], t_s.at[i - 1], t_r.at[i - 1], dev))
        bulk.append(send(dist_ref.at[j], D.at[0, me], d_s.at[i - 1], d_r.at[i - 1], dev))
        bulk.append(send(W.at[me], W.at[me], w_s.at[i - 1], w_r.at[i - 1], dev))
    for c in bulk:
        c.start()

    total_rows = NB * degree
    shift_nodes = (node_count - 1).bit_length()
    assert 1 << shift_nodes == node_count
    path = path_ref[...]
    slot_of = path >> shift_nodes
    node_of = path & (node_count - 1)
    row_of = (node_of >> 7) * degree + slot_of
    lane_of = node_of & (LANES - 1)
    row_iota = lax.broadcasted_iota(jnp.int32, (total_rows, LANES), 0)
    lane_iota = lax.broadcasted_iota(jnp.int32, (LANES, LANES), 0)
    acc = jnp.zeros((total_rows, LANES), jnp.float32)
    for k in range(path.shape[0]):
        hi = jnp.where(row_iota == row_of[k:k + 1, :], 1.0, 0.0).astype(jnp.bfloat16)
        lo = jnp.where(lane_iota == lane_of[k:k + 1, :], 1.0, 0.0).astype(jnp.bfloat16)
        count = lax.dot_general(hi, lo, (((1,), (1,)), ((), ())), preferred_element_type=jnp.float32)
        acc = acc + count * demand_ref[k]
    F[...] = acc.reshape(F.shape)

    for c in bulk:
        c.wait_recv()

    sub_iota = lax.broadcasted_iota(jnp.int32, (rows, LANES), 0)
    lane_row = lax.broadcasted_iota(jnp.int32, (rows, LANES), 1)
    source = jnp.zeros((rows, LANES), jnp.int32)
    for r in range(rows):
        source = jnp.where(sub_iota == r, source_ref[me * rows + r], source)
    def prepare(j, _):
        for h in range(m):
            lanes = slice(h * LANES, (h + 1) * LANES)
            vb = j * m + h
            D[0, j, :, lanes] = jnp.where(lane_row + vb * LANES == source, 0.0, D[0, j, :, lanes])
            tail = T[j, :, lanes]
            rel = (tail >> 7) - vb + REACH
            rel = jnp.where(rel < 0, rel + NB, rel)
            rel = jnp.where(rel >= NB, rel - NB, rel)
            CODE[j, :, lanes] = rel
            T[j, :, lanes] = tail & (LANES - 1)
        return 0

    for c in bulk:
        c.wait_send()
    lax.fori_loop(0, A, prepare, 0)

    flows = []
    for i in range(1, A):
        j = arc_dev(i)
        flows.append(send(F.at[j], RF.at[me], f_s.at[i - 1], f_r.at[i - 1], (mc, j)))
    for c in flows:
        c.start()

    sub8 = lax.broadcasted_iota(jnp.int32, (8, LANES), 0)
    halves = [(sub8 & d) == 0 for d in (4, 2, 1)]

    def min_over_slots(parts):
        parts = parts + [parts[-1]] * (8 - len(parts))
        for mask, d in zip(halves, (4, 2, 1)):
            merged = []
            for lower, upper in zip(parts[:d], parts[d:]):
                kept = jnp.where(mask, lower, upper)
                other = jnp.where(mask, upper, lower)
                moved = pltpu.roll(other, d, 0)
                if d != 4:
                    moved = jnp.where(mask, pltpu.roll(other, 8 - d, 0), moved)
                merged.append(jnp.minimum(kept, moved))
            parts = merged
        return parts[0]

    def relax_block(read, write, j):
        for h in range(m):
            lanes = slice(h * LANES, (h + 1) * LANES)
            where_from = []
            for off in range(-REACH, REACH + 1):
                q = h + off
                blk = q % m
                where_from.append((lax.rem(j + (q // m) % A, A), slice(blk * LANES, (blk + 1) * LANES)))
            groups = [slice(g, g + 8) for g in range(0, degree, 8)]
            idx = [T[j, g, lanes] for g in groups]
            weight = [W[j, g, lanes] for g in groups]
            code = [CODE[j, g, lanes] for g in groups]
            masks = [[c == b for b in range(2 * REACH)] for c in code]
            cand = [None] * rows
            for g in range(len(groups)):
                for r in range(rows):
                    srcs = [jnp.broadcast_to(D[read, jj, r:r + 1, bl], (8, LANES)) for jj, bl in where_from]
                    got = [jnp.take_along_axis(x, idx[g], axis=1, mode="promise_in_bounds") for x in srcs]
                    pick = got[2 * REACH]
                    for b in range(2 * REACH):
                        pick = jnp.where(masks[g][b], got[b], pick)
                    pick = pick + weight[g]
                    cand[r] = pick if cand[r] is None else jnp.minimum(cand[r], pick)
            for first in range(0, rows, 8):
                last = min(first + 8, rows)
                best = min_over_slots(cand[first:last])[:last - first]
                D[write, j, first:last, lanes] = jnp.minimum(D[read, j, first:last, lanes], best)

    def sweeps(first, last):
        def one(t, _):
            read = lax.rem(t, 2)
            def blk(j, _):
                relax_block(read, 1 - read, j)
                return 0
            lax.fori_loop(0, A, blk, 0, unroll=UNROLL)
            return 0
        lax.fori_loop(first, last, one, 0)

    sweeps(0, 2)
    for c in flows:
        c.wait()
    total = F[me]
    for i in range(1, A):
        total = total + RF[arc_dev(i)]
    G[mc] = total
    sweeps(2, 3)
    groups = [send(G.at[mc], G.at[mc], g_s.at[i - 1], g_r.at[i - 1], (comm_dev(i), me)) for i in range(1, C)]
    for c in groups:
        c.start()
    sweeps(3, 5)
    for c in groups:
        c.wait()
    flow = G[0]
    for i in range(1, C):
        flow = flow + G[i]
    gradient = [flow[h * degree:(h + 1) * degree, :] - cap_ref[:, h * LANES:(h + 1) * LANES] for h in range(m)]
    square = sum(g * g for g in gradient)
    Q[me] = square
    sweeps(5, 6)
    norms = [send(Q.at[me], Q.at[me], q_s.at[i - 1], q_r.at[i - 1], (mc, arc_dev(i))) for i in range(1, A)]
    for c in norms:
        c.start()
    sweeps(6, SWEEPS - 1)
    for c in norms:
        c.wait()
    square = Q[0]
    for i in range(1, A):
        square = square + Q[i]
    scale_root = jnp.sqrt(jnp.sum(square) / (degree * node_count) + eps_value)
    for h in range(m):
        lanes = slice(h * LANES, (h + 1) * LANES)
        newp_ref[:, lanes] = jnp.maximum(price_ref[:, lanes] + step_size * gradient[h] / scale_root, 0.0)

    read = (SWEEPS - 1) % 2
    outs = [send(D.at[1 - read, arc_dev(i)], out_ref.at[me], o_s.at[i - 1], o_r.at[i - 1], (mc, arc_dev(i)))
            for i in range(1, A)]
    for i in range(1, A + 1):
        relax_block(read, 1 - read, arc_dev(i))
        if i >= 2:
            outs[i - 2].start()
    out_ref[me] = D[1 - read, me]
    for c in outs:
        c.wait()


def shards(A, C, prev_dist, source_node, arc_tail, base_cost, arc_price, capacity, path_arcs, demand):
    commodities, span = prev_dist.shape
    degree = arc_tail.shape[0]
    rows = commodities // A
    m = span // LANES
    f32 = jnp.float32
    vmem = pl.BlockSpec(memory_space=pltpu.VMEM)
    smem = pl.BlockSpec(memory_space=pltpu.SMEM)
    sems = pltpu.SemaphoreType.DMA
    out, new_price = pl.pallas_call(
        functools.partial(kernel, A, C, m),
        out_shape=(jax.ShapeDtypeStruct((A, rows, span), f32), jax.ShapeDtypeStruct((degree, span), f32)),
        in_specs=[smem, smem] + [vmem] * 6,
        out_specs=(vmem, vmem),
        scratch_shapes=[
            pltpu.VMEM((2, A, rows, span), f32),
            pltpu.VMEM((A, degree, span), jnp.int32),
            pltpu.VMEM((A, degree, span), f32),
            pltpu.VMEM((A, degree, span), jnp.int32),
            pltpu.VMEM((A, m * degree, LANES), f32),
            pltpu.VMEM((A, m * degree, LANES), f32),
            pltpu.VMEM((C, m * degree, LANES), f32),
            pltpu.VMEM((A, degree, LANES), f32),
        ] + [sems((A - 1,))] * 8 + [sems((C - 1,))] * 2 + [sems((A - 1,))] * 4,
        compiler_params=pltpu.CompilerParams(collective_id=0, has_side_effects=True),
    )(source_node, demand, prev_dist.reshape(A, rows, span), arc_tail, base_cost, arc_price, capacity, path_arcs)
    return (out.reshape(commodities, span), new_price)


def solution(mesh):
    in_specs = (
        P("comm", "arc"),
        P("comm"),
        P(None, "arc"),
        P(None, "arc"),
        P(None, "arc"),
        P(None, "arc"),
        P(("comm", "arc"), None),
        P(("comm", "arc")),
    )
    out_specs = (P("comm", "arc"), P(None, "arc"))
    body = functools.partial(shards, mesh.shape["arc"], mesh.shape["comm"])
    return jax.shard_map(body, mesh=mesh, in_specs=in_specs, out_specs=out_specs, check_vma=False)
```

```python
import functools

import jax
import jax.numpy as jnp
from jax import lax
from jax.experimental import pallas as pl
from jax.experimental.pallas import tpu as pltpu
from jax.sharding import PartitionSpec as P

SWEEPS = 8
LANES = 128
REACH = 2
UNROLL = 4

step_size = 0.25
eps_value = 1e-06
MESH_ID = pl.DeviceIdType.MESH


def kernel(A, C, m,
           source_ref, demand_ref, dist_ref, tail_ref, cost_ref, price_ref, cap_ref, path_ref,
           out_ref, newp_ref,
           D, T, W, CODE, F, RF, G, Q,
           d_s, d_r, t_s, t_r, w_s, w_r, f_s, f_r, g_s, g_r, q_s, q_r, o_s, o_r):
    rows = D.shape[2]
    degree, span = tail_ref.shape
    NB = A * m
    node_count = NB * LANES
    me = lax.axis_index("arc")
    mc = lax.axis_index("comm")

    def arc_dev(i):
        return lax.rem(me + i, A)

    def comm_dev(i):
        return lax.rem(mc + i, C)

    W[me] = cost_ref[...] + price_ref[...]
    T[me] = tail_ref[...]
    D[0, me] = dist_ref[me]

    barrier = pltpu.get_barrier_semaphore()
    for i in range(1, A):
        pl.semaphore_signal(barrier, inc=1, device_id=(mc, arc_dev(i)), device_id_type=MESH_ID)
    for i in range(1, C):
        pl.semaphore_signal(barrier, inc=1, device_id=(comm_dev(i), me), device_id_type=MESH_ID)
    pl.semaphore_wait(barrier, A - 1 + C - 1)

    def send(src, dst, ss, rs, dev):
        return pltpu.make_async_remote_copy(src_ref=src, dst_ref=dst, send_sem=ss, recv_sem=rs,
                                            device_id=dev, device_id_type=MESH_ID)

    bulk = []
    for i in range(1, A):
        j = arc_dev(i)
        dev = (mc, j)
        bulk.append(send(tail_ref, T.at[me], t_s.at[i - 1], t_r.at[i - 1], dev))
        bulk.append(send(dist_ref.at[j], D.at[0, me], d_s.at[i - 1], d_r.at[i - 1], dev))
        bulk.append(send(W.at[me], W.at[me], w_s.at[i - 1], w_r.at[i - 1], dev))
    for c in bulk:
        c.start()

    total_rows = NB * degree
    shift_nodes = (node_count - 1).bit_length()
    assert 1 << shift_nodes == node_count
    path = path_ref[...]
    slot_of = path >> shift_nodes
    node_of = path & (node_count - 1)
    row_of = (node_of >> 7) * degree + slot_of
    lane_of = node_of & (LANES - 1)
    row_iota = lax.broadcasted_iota(jnp.int32, (total_rows, LANES), 0)
    lane_iota = lax.broadcasted_iota(jnp.int32, (LANES, LANES), 0)
    acc = jnp.zeros((total_rows, LANES), jnp.float32)
    for k in range(path.shape[0]):
        hi = jnp.where(row_iota == row_of[k:k + 1, :], 1.0, 0.0).astype(jnp.bfloat16)
        lo = jnp.where(lane_iota == lane_of[k:k + 1, :], 1.0, 0.0).astype(jnp.bfloat16)
        count = lax.dot_general(hi, lo, (((1,), (1,)), ((), ())), preferred_element_type=jnp.float32)
        acc = acc + count * demand_ref[k]
    F[...] = acc.reshape(F.shape)

    for c in bulk:
        c.wait_recv()

    sub_iota = lax.broadcasted_iota(jnp.int32, (rows, LANES), 0)
    lane_row = lax.broadcasted_iota(jnp.int32, (rows, LANES), 1)
    source = jnp.zeros((rows, LANES), jnp.int32)
    for r in range(rows):
        source = jnp.where(sub_iota == r, source_ref[me * rows + r], source)
    def prepare(j, _):
        for h in range(m):
            lanes = slice(h * LANES, (h + 1) * LANES)
            vb = j * m + h
            D[0, j, :, lanes] = jnp.where(lane_row + vb * LANES == source, 0.0, D[0, j, :, lanes])
            tail = T[j, :, lanes]
            rel = (tail >> 7) - vb + REACH
            rel = jnp.where(rel < 0, rel + NB, rel)
            rel = jnp.where(rel >= NB, rel - NB, rel)
            CODE[j, :, lanes] = rel
            T[j, :, lanes] = tail & (LANES - 1)
        return 0

    for c in bulk:
        c.wait_send()
    lax.fori_loop(0, A, prepare, 0)

    flows = []
    for i in range(1, A):
        j = arc_dev(i)
        flows.append(send(F.at[j], RF.at[me], f_s.at[i - 1], f_r.at[i - 1], (mc, j)))
    for c in flows:
        c.start()

    sub8 = lax.broadcasted_iota(jnp.int32, (8, LANES), 0)
    halves = [(sub8 & d) == 0 for d in (4, 2, 1)]

    def min_over_slots(parts):
        parts = parts + [parts[-1]] * (8 - len(parts))
        for mask, d in zip(halves, (4, 2, 1)):
            merged = []
            for lower, upper in zip(parts[:d], parts[d:]):
                kept = jnp.where(mask, lower, upper)
                other = jnp.where(mask, upper, lower)
                moved = pltpu.roll(other, d, 0)
                if d != 4:
                    moved = jnp.where(mask, pltpu.roll(other, 8 - d, 0), moved)
                merged.append(jnp.minimum(kept, moved))
            parts = merged
        return parts[0]

    def relax_block(read, write, j, pending):
        for h in range(m):
            lanes = slice(h * LANES, (h + 1) * LANES)
            where_from = []
            for off in range(-REACH, REACH + 1):
                q = h + off
                blk = q % m
                where_from.append((lax.rem(j + (q // m) % A, A), slice(blk * LANES, (blk + 1) * LANES)))
            groups = [slice(g, g + 8) for g in range(0, degree, 8)]
            idx = [T[j, g, lanes] for g in groups]
            weight = [W[j, g, lanes] for g in groups]
            code = [CODE[j, g, lanes] for g in groups]
            masks = [[c == b for b in range(2 * REACH)] for c in code]
            for n, first in enumerate(range(0, rows, 8)):
                last = min(first + 8, rows)
                got = {}
                order = range(len(groups)) if n % 2 == 0 else range(len(groups) - 1, -1, -1)
                for g in order:
                    for r in range(first, last):
                        got[g, r] = [jnp.take_along_axis(
                            jnp.broadcast_to(D[read, jj, r:r + 1, bl], (8, LANES)), idx[g],
                            axis=1, mode="promise_in_bounds") for jj, bl in where_from]
                old = D[read, j, first:last, lanes]
                if pending:
                    pending.pop()()

                def finish(got=got, order=order, masks=masks, weight=weight, first=first, last=last,
                           old=old, j=j, lanes=lanes):
                    cand = {}
                    for g in order:
                        for r in range(first, last):
                            pick = got[g, r][2 * REACH]
                            for b in range(2 * REACH):
                                pick = jnp.where(masks[g][b], got[g, r][b], pick)
                            pick = pick + weight[g]
                            cand[r] = jnp.minimum(cand[r], pick) if r in cand else pick
                    best = min_over_slots([cand[r] for r in range(first, last)])[:last - first]
                    D[write, j, first:last, lanes] = jnp.minimum(old, best)

                pending.append(finish)

    def sweeps(first, last):
        def one(t, _):
            read = lax.rem(t, 2)
            def blk(jo, _):
                pending = []
                for u in range(UNROLL):
                    relax_block(read, 1 - read, jo * UNROLL + u, pending)
                pending.pop()()
                return 0
            assert A % UNROLL == 0
            lax.fori_loop(0, A // UNROLL, blk, 0)
            return 0
        lax.fori_loop(first, last, one, 0)

    sweeps(0, 2)
    for c in flows:
        c.wait()
    total = F[me]
    for i in range(1, A):
        total = total + RF[arc_dev(i)]
    G[mc] = total
    sweeps(2, 3)
    groups = [send(G.at[mc], G.at[mc], g_s.at[i - 1], g_r.at[i - 1], (comm_dev(i), me)) for i in range(1, C)]
    for c in groups:
        c.start()
    sweeps(3, 5)
    for c in groups:
        c.wait()
    flow = G[0]
    for i in range(1, C):
        flow = flow + G[i]
    gradient = [flow[h * degree:(h + 1) * degree, :] - cap_ref[:, h * LANES:(h + 1) * LANES] for h in range(m)]
    square = sum(g * g for g in gradient)
    Q[me] = square
    sweeps(5, 6)
    norms = [send(Q.at[me], Q.at[me], q_s.at[i - 1], q_r.at[i - 1], (mc, arc_dev(i))) for i in range(1, A)]
    for c in norms:
        c.start()
    sweeps(6, SWEEPS - 1)
    for c in norms:
        c.wait()
    square = Q[0]
    for i in range(1, A):
        square = square + Q[i]
    scale_root = jnp.sqrt(jnp.sum(square) / (degree * node_count) + eps_value)
    for h in range(m):
        lanes = slice(h * LANES, (h + 1) * LANES)
        newp_ref[:, lanes] = jnp.maximum(price_ref[:, lanes] + step_size * gradient[h] / scale_root, 0.0)

    read = (SWEEPS - 1) % 2
    outs = [send(D.at[1 - read, arc_dev(i)], out_ref.at[me], o_s.at[i - 1], o_r.at[i - 1], (mc, arc_dev(i)))
            for i in range(1, A)]
    for i in range(1, A + 1):
        pending = []
        relax_block(read, 1 - read, arc_dev(i), pending)
        pending.pop()()
        if i >= 2:
            outs[i - 2].start()
    out_ref[me] = D[1 - read, me]
    for c in outs:
        c.wait()


def shards(A, C, prev_dist, source_node, arc_tail, base_cost, arc_price, capacity, path_arcs, demand):
    commodities, span = prev_dist.shape
    degree = arc_tail.shape[0]
    rows = commodities // A
    m = span // LANES
    f32 = jnp.float32
    vmem = pl.BlockSpec(memory_space=pltpu.VMEM)
    smem = pl.BlockSpec(memory_space=pltpu.SMEM)
    sems = pltpu.SemaphoreType.DMA
    out, new_price = pl.pallas_call(
        functools.partial(kernel, A, C, m),
        out_shape=(jax.ShapeDtypeStruct((A, rows, span), f32), jax.ShapeDtypeStruct((degree, span), f32)),
        in_specs=[smem, smem] + [vmem] * 6,
        out_specs=(vmem, vmem),
        scratch_shapes=[
            pltpu.VMEM((2, A, rows, span), f32),
            pltpu.VMEM((A, degree, span), jnp.int32),
            pltpu.VMEM((A, degree, span), f32),
            pltpu.VMEM((A, degree, span), jnp.int32),
            pltpu.VMEM((A, m * degree, LANES), f32),
            pltpu.VMEM((A, m * degree, LANES), f32),
            pltpu.VMEM((C, m * degree, LANES), f32),
            pltpu.VMEM((A, degree, LANES), f32),
        ] + [sems((A - 1,))] * 8 + [sems((C - 1,))] * 2 + [sems((A - 1,))] * 4,
        compiler_params=pltpu.CompilerParams(collective_id=0, has_side_effects=True),
    )(source_node, demand, prev_dist.reshape(A, rows, span), arc_tail, base_cost, arc_price, capacity, path_arcs)
    return (out.reshape(commodities, span), new_price)


def solution(mesh):
    in_specs = (
        P("comm", "arc"),
        P("comm"),
        P(None, "arc"),
        P(None, "arc"),
        P(None, "arc"),
        P(None, "arc"),
        P(("comm", "arc"), None),
        P(("comm", "arc")),
    )
    out_specs = (P("comm", "arc"), P(None, "arc"))
    body = functools.partial(shards, mesh.shape["arc"], mesh.shape["comm"])
    return jax.shard_map(body, mesh=mesh, in_specs=in_specs, out_specs=out_specs, check_vma=False)
```
